32 devices in a mesh: rack: 4 (over x, core), chip: 8 (over z, y).
Axes of the slice: x: 2, y: 2, z: 4, core: 2. Of those that a mesh axis runs over, the one named last changes fastest.
Arguments:
- points: float32 [64, 4, 32, 256], P(('rack', 'chip')), may hold values from -6 to 6
- counts: int32 [64, 256], P(('rack', 'chip')), may hold values from 1 to 32
- cells: int32 [64, 256], P(('rack', 'chip')), may hold values from 0 to 2047, as said below
- pfn_weight: float32 [9, 64], replicated, may hold values from -2 to 2
- pfn_gain: float32 [64], replicated, may hold values from 0.5 to 1.5
- pfn_bias: float32 [64], replicated, may hold values from -3 to 3
- conv_weight: float32 [4, 9, 4096], replicated, may hold values from -0.25 to 0.25
- bn_gain: float32 [4, 64], replicated, may hold values from 0.5 to 1.5
- bn_bias: float32 [4, 64], replicated, may hold values from -3 to 3
- cotangent: float32 [64, 64, 4, 128], P(('rack', 'chip')), may hold values from -0.006 to 0.006
Outputs:
- features: float32 [64, 64, 4, 128], P(('rack', 'chip'))
- conv_grads: float32 [4, 9, 4096], replicated
- norm_grads: float32 [2, 4, 64], replicated
- pillar_grad: float32 [64, 64, 256], P(('rack', 'chip'))
The draws below stay inside these ranges and needn't reach their ends.
Inputs may be any that keep to these rules, and one draw needn't show every extreme that they name: `cells`: within one sweep no two pillars share a cell.
All inputs are finite; a program needn't handle non-finite values.
Results may differ from the reference program's by a relative error of at most 0.0003.
Values sent between devices are 32-bit elements; how exact they have to be, the bound alone decides.
A program may use at most 128 MiB of HBM per device.

```python
import jax
import jax.numpy as jnp
from jax import lax

C = 64
MAXP = 32
LAYERS = 4
GH = 8
GW = 256
PILL = 256
SWEEPS = 64


def draw_cells(key, part):
    keys = jax.random.split(key, SWEEPS)

    def one_sweep(sweep_key):
        return jax.random.permutation(sweep_key, GH * GW)[:PILL].astype(jnp.int32)
    return jax.vmap(one_sweep)(keys)


def touch_ends(values, own_key, least, largest):
    dims = values.shape
    spot = [jax.random.randint(jax.random.fold_in(own_key, axis), (), 0, dims[axis]) for axis in range(len(dims))]
    values = values.at[tuple(spot)].set(least)
    longest = dims.index(max(dims))
    spot[longest] = (spot[longest] + 1) % dims[longest]
    return values.at[tuple(spot)].set(largest)


def steps_of(rng, dims, pieces, smallest, largest):
    def one(axis_at, shards_of):
        heights = jax.random.uniform(jax.random.fold_in(jax.random.fold_in(rng, 6), axis_at), (shards_of,), jnp.float32, smallest / len(pieces), largest / len(pieces))
        return jnp.repeat(jnp.exp(heights), dims[axis_at] // shards_of).reshape((-1,) + (1,) * (len(dims) - axis_at - 1))

    level = one(*pieces[0])
    for cut in pieces[1:]:
        level = level * one(*cut)
    return level


def bell_draw(own_key, shape, spread, bound, pieces=(), kind=jnp.bfloat16):
    values = jax.random.normal(own_key, shape, jnp.float32) * spread
    if len(pieces) > 0:
        values = steps_of(own_key, shape, pieces, -0.22, 0.18) * values
    return jnp.clip(values, min=-bound, max=bound).astype(kind)


def setup_inputs(seed: int = 0) -> dict:
    streams_of = jax.random.split(jax.random.key(seed), 11)
    points = bell_draw(streams_of[0], (SWEEPS, 4, MAXP, PILL), 1.0, 6.0, ((0, 32),), jnp.float32)
    counts = touch_ends(jax.random.randint(streams_of[1], (SWEEPS, PILL), 1, MAXP + 1), jax.random.fold_in(streams_of[1], 1), 1, MAXP).astype(jnp.int32)
    cells = draw_cells(jax.random.fold_in(streams_of[10], 71), 0)
    pfn_weight = bell_draw(streams_of[3], (9, C), 9 ** -0.5, 2.0, (), jnp.float32)
    pfn_gain = jnp.clip(1.0 + 0.1 * jax.random.normal(streams_of[4], (C,), jnp.float32), 0.5, 1.5)
    pfn_bias = bell_draw(streams_of[5], (C,), 0.5, 3.0, (), jnp.float32)
    conv_weight = bell_draw(streams_of[6], (LAYERS, 9, C * C), (9 * C) ** -0.5, 0.25, (), jnp.float32)
    bn_gain = jnp.clip(1.0 + 0.1 * jax.random.normal(streams_of[7], (LAYERS, C), jnp.float32), 0.5, 1.5)
    bn_bias = bell_draw(streams_of[8], (LAYERS, C), 0.5, 3.0, (), jnp.float32)
    cotangent = bell_draw(streams_of[9], (SWEEPS, C, GH // 2, GW // 2), 0.001, 0.006, ((0, 32),), jnp.float32)
    return dict(points=points, counts=counts, cells=cells, pfn_weight=pfn_weight, pfn_gain=pfn_gain, pfn_bias=pfn_bias, conv_weight=conv_weight, bn_gain=bn_gain, bn_bias=bn_bias, cotangent=cotangent)


EPS = 1e-05
PRECISE = lax.Precision.HIGHEST

def channel_shape(vector, ndim):
    return vector.reshape((1, -1) + (1,) * (ndim - 2))

def silu_slope(pre_act):
    sigma = jax.nn.sigmoid(pre_act)
    return sigma * (1.0 + pre_act * (1.0 - sigma))

def pillar_hidden(points, counts, cells, pfn_weight):
    slot_ids = lax.broadcasted_iota(jnp.int32, (1, points.shape[2], 1), 1)
    is_valid = (slot_ids < counts[:, None, :]).astype(jnp.float32)
    point_count = counts.astype(jnp.float32)
    centroid = lax.optimization_barrier(jnp.sum(points[:, 0:3] * is_valid[:, None], axis=2)) / point_count[:, None]
    col_pos = (cells % GW).astype(jnp.float32) * (2.0 / GW) - 1.0
    row_pos = (cells // GW).astype(jnp.float32) * (2.0 / GH) - 1.0
    offsets = points[:, 0:3] - centroid[:, :, None, :]
    grid_off = jnp.stack([points[:, 0] - col_pos[:, None, :], points[:, 1] - row_pos[:, None, :]], axis=1)
    inputs = jnp.concatenate([points, offsets, grid_off], axis=1)
    hidden = jnp.einsum('fc,sfpq->scpq', pfn_weight, inputs, precision=PRECISE)
    return (hidden, is_valid)

def normalize_pillars(hidden, is_valid, mean_val, inv_std, gain, bias):
    scaled = channel_shape(gain, 4) * (hidden - channel_shape(mean_val, 4)) * channel_shape(inv_std, 4) + channel_shape(bias, 4)
    return lax.optimization_barrier(jnp.max(jnp.maximum(scaled, 0.0) * is_valid[:, None], axis=2))

def scatter_pillars(pillar, cells):
    empty = jnp.zeros((pillar.shape[1], GH * GW), pillar.dtype)
    placed = jax.vmap(lambda feature, target: empty.at[:, target].set(feature))(pillar, cells)
    return placed.reshape(pillar.shape[0], pillar.shape[1], GH, GW)

def conv_forward(activation, taps, stride):
    padded = jnp.pad(activation, ((0, 0), (0, 0), (1, 1), (1, 1)))
    height = activation.shape[2] // stride
    width = activation.shape[3] // stride
    result = jnp.zeros((activation.shape[0], C, height, width), jnp.float32)
    for row_tap in range(3):
        for col_tap in range(3):
            tap_slice = padded[:, :, row_tap:row_tap + stride * height:stride, col_tap:col_tap + stride * width:stride]
            kernel = taps[3 * row_tap + col_tap].reshape(C, C)
            result = result + jnp.einsum('oi,nihw->nohw', kernel, tap_slice, precision=PRECISE)
    return result

def conv_backward(activation, taps, grad_z, stride):
    padded = jnp.pad(activation, ((0, 0), (0, 0), (1, 1), (1, 1)))
    height = grad_z.shape[2]
    width = grad_z.shape[3]
    grad_pad = jnp.zeros(padded.shape, jnp.float32)
    tap_grads = []
    for row_tap in range(3):
        for col_tap in range(3):
            tap_slice = padded[:, :, row_tap:row_tap + stride * height:stride, col_tap:col_tap + stride * width:stride]
            tap_grads.append(jnp.einsum('nohw,nihw->oi', grad_z, tap_slice, precision=PRECISE).reshape(C * C))
            kernel = taps[3 * row_tap + col_tap].reshape(C, C)
            back = jnp.einsum('oi,nohw->nihw', kernel, grad_z, precision=PRECISE)
            grad_pad = grad_pad.at[:, :, row_tap:row_tap + stride * height:stride, col_tap:col_tap + stride * width:stride].add(back)
    return (jnp.stack(tap_grads), grad_pad[:, :, 1:-1, 1:-1])

def reference(points, counts, cells, pfn_weight, pfn_gain, pfn_bias, conv_weight, bn_gain, bn_bias, cotangent):

    def hidden_of(args):
        return pillar_hidden(args[0][None], args[1][None], args[2][None], pfn_weight)

    def first_sums(args):
        hidden, is_valid = hidden_of(args)
        return (lax.optimization_barrier(jnp.sum(hidden * is_valid[:, None], axis=(0, 2, 3))), jnp.sum(is_valid))
    totals, counts_each = lax.map(first_sums, (points, counts, cells))
    count_all = jnp.sum(counts_each)
    mean_val = lax.optimization_barrier(jnp.sum(totals, axis=0)) / count_all

    def second_sums(args):
        hidden, is_valid = hidden_of(args)
        centred = hidden - channel_shape(mean_val, 4)
        return lax.optimization_barrier(jnp.sum(centred * centred * is_valid[:, None], axis=(0, 2, 3)))
    variance = lax.optimization_barrier(jnp.sum(lax.map(second_sums, (points, counts, cells)), axis=0)) / count_all
    inv_std = lax.rsqrt(variance + EPS)

    def to_grid(args):
        hidden, is_valid = hidden_of(args)
        pillar = normalize_pillars(hidden, is_valid, mean_val, inv_std, pfn_gain, pfn_bias)
        return scatter_pillars(pillar, args[2][None])[0]
    bev_grid = lax.map(to_grid, (points, counts, cells))
    activations = [bev_grid]
    normals = []
    for layer_idx in range(LAYERS):
        stride = 2 if layer_idx == 0 else 1
        weight = conv_weight[layer_idx]
        pre_norm = lax.map(lambda sweep: conv_forward(sweep[None], weight, stride)[0], activations[-1])
        mean_c = lax.optimization_barrier(jnp.mean(pre_norm, axis=(0, 2, 3)))
        centred = pre_norm - channel_shape(mean_c, 4)
        inv_c = lax.rsqrt(lax.optimization_barrier(jnp.mean(centred * centred, axis=(0, 2, 3))) + EPS)
        normed = centred * channel_shape(inv_c, 4)
        scaled = channel_shape(bn_gain[layer_idx], 4) * normed + channel_shape(bn_bias[layer_idx], 4)
        activations.append(jax.nn.silu(scaled))
        normals.append((normed, inv_c, scaled))
    upstream = cotangent
    grad_list = [None] * LAYERS
    gain_list = [None] * LAYERS
    bias_list = [None] * LAYERS
    pillar_grad = None
    for layer_idx in range(LAYERS - 1, -1, -1):
        stride = 2 if layer_idx == 0 else 1
        weight = conv_weight[layer_idx]
        normed, inv_c, scaled = normals[layer_idx]
        grad_y = upstream * silu_slope(scaled)
        sum_dy = lax.optimization_barrier(jnp.sum(grad_y, axis=(0, 2, 3)))
        sum_dyx = lax.optimization_barrier(jnp.sum(grad_y * normed, axis=(0, 2, 3)))
        entries = float(grad_y.shape[0] * grad_y.shape[2] * grad_y.shape[3])
        grad_z = channel_shape(bn_gain[layer_idx] * inv_c, 4) * (grad_y - channel_shape(sum_dy / entries, 4) - normed * channel_shape(sum_dyx / entries, 4))
        if layer_idx == 0:

            def back_first(args):
                grad_w, grad_in = conv_backward(args[0][None], weight, args[1][None], stride)
                plane = grad_in[0].reshape(grad_in.shape[1], GH * GW)
                return (grad_w, plane[:, args[2]])
            parts, pillar_grad = lax.map(back_first, (activations[0], grad_z, cells))
        else:

            def back_other(args):
                grad_w, grad_in = conv_backward(args[0][None], weight, args[1][None], stride)
                return (grad_w, grad_in[0])
            parts, upstream = lax.map(back_other, (activations[layer_idx], grad_z))
        grad_list[layer_idx] = lax.optimization_barrier(jnp.sum(parts, axis=0))
        gain_list[layer_idx] = sum_dyx
        bias_list[layer_idx] = sum_dy
    norm_grads = jnp.stack([jnp.stack(gain_list), jnp.stack(bias_list)])
    return (activations[-1], jnp.stack(grad_list), norm_grads, pillar_grad)
```

```python
import functools

import jax
import jax.numpy as jnp
from jax import lax
from jax.experimental import pallas as pl
from jax.experimental.pallas import tpu as pltpu
from jax.sharding import PartitionSpec as P

LAYERS = 4
EPS = 1e-05
F32 = jnp.float32
BF16 = jnp.bfloat16
NN = (((1,), (0,)), ((), ()))
NT = (((1,), (1,)), ((), ()))
LOWEST = -3e38


def dot(a, b, dims=NN):
    return lax.dot_general(a, b, dims, preferred_element_type=F32)


def split(x):
    hi = x.astype(BF16)
    lo = (x - hi.astype(F32)).astype(BF16)
    return hi, lo


def kernel(
    dims,
    points,
    counts,
    cells,
    pw_s,
    pw_t,
    pfn_gb,
    wf,
    wb,
    wb0,
    bn_cols,
    cot,
    feat,
    grads,
    norms,
    pgrad,
    xs,
    gs,
    wfs,
    wbs,
    wb0s,
    onehot,
    bm,
    mx,
    sq,
    xh,
    yy,
    gz_s,
    st0,
    st,
    rs,
    rbuf,
    st_send,
    st_recv,
    rs_send,
    rs_recv,
    ag_send,
    ag_recv,
):
    n_rack, n_chip, sweeps, maxp, gh, gw, pill, ch, owners = dims
    n = n_rack * n_chip
    h2, w2 = gh // 2, gw // 2
    plane = h2 * w2
    pix = sweeps * plane
    rows_per = ch // owners
    kdim = 9 * ch
    me = lax.axis_index("rack") * n_chip + lax.axis_index("chip")

    def device(t):
        return {"rack": lax.div(t, n_chip), "chip": lax.rem(t, n_chip)}

    def peers(body):
        def step(k, carry):
            body(lax.rem(me + k, n))
            return carry

        lax.fori_loop(1, n, step, 0)

    barrier = pltpu.get_barrier_semaphore()
    peers(
        lambda t: pl.semaphore_signal(
            barrier, inc=1, device_id=device(t), device_id_type=pl.DeviceIdType.MESH
        )
    )

    def send_row(buf, rnd, row):
        buf[rnd, me] = row

        def go(t):
            pltpu.make_async_remote_copy(
                src_ref=buf.at[rnd, me],
                dst_ref=buf.at[rnd, me],
                send_sem=st_send.at[rnd],
                recv_sem=st_recv.at[rnd],
                device_id=device(t),
                device_id_type=pl.DeviceIdType.MESH,
            ).start()

        peers(go)

    def wait_row(buf, rnd):
        most = buf.at[rnd, pl.ds(0, n - 1)]
        pltpu.make_async_copy(most, most, st_recv.at[rnd]).wait()
        return buf[rnd]

    def send_parts(layer):
        def go(t):
            def copy():
                pltpu.make_async_remote_copy(
                    src_ref=rs.at[layer, t],
                    dst_ref=rbuf.at[layer, me],
                    send_sem=rs_send.at[layer],
                    recv_sem=rs_recv.at[layer],
                    device_id=device(t),
                    device_id_type=pl.DeviceIdType.MESH,
                ).start()

            if owners == n:
                copy()
            else:
                pl.when(t < owners)(copy)

        peers(go)

    def when_owner(body):
        if owners == n:
            body()
        else:
            pl.when(me < owners)(body)

    def add_parts(layer):
        def body():
            most = rbuf.at[layer, pl.ds(0, n - 1)]
            pltpu.make_async_copy(most, most, rs_recv.at[layer]).wait()
            rbuf[layer, me] = rs[layer, me]
            grads[layer, me] = jnp.sum(rbuf[layer], axis=0)

            def go(t):
                pltpu.make_async_remote_copy(
                    src_ref=grads.at[layer, me],
                    dst_ref=grads.at[layer, me],
                    send_sem=ag_send.at[layer],
                    recv_sem=ag_recv.at[layer],
                    device_id=device(t),
                    device_id_type=pl.DeviceIdType.MESH,
                ).start()

            peers(go)

        when_owner(body)

    slot = lax.broadcasted_iota(jnp.int32, (maxp, pill), 0)
    lane = lax.broadcasted_iota(jnp.int32, (1, 2 * ch), 1)
    per_sweep = []
    totals = [jnp.zeros((1, 1), F32)] * 9
    n_loc = jnp.zeros((1, 1), F32)
    for s in range(sweeps):
        valid = slot < counts[s : s + 1, :]
        mask = valid.astype(F32)
        cnt = counts[s : s + 1, :].astype(F32)
        sums = [jnp.sum(points[s, f] * mask, axis=0, keepdims=True) for f in range(4)]
        cents = [sums[f] / cnt for f in range(3)]
        cell = cells[s : s + 1, :]
        row = lax.shift_right_logical(cell, gw.bit_length() - 1)
        col = cell & (gw - 1)
        col_pos = col.astype(F32) * (2.0 / gw) - 1.0
        row_pos = row.astype(F32) * (2.0 / gh) - 1.0
        feats = sums + [sums[f] - cnt * cents[f] for f in range(3)]
        feats += [sums[0] - cnt * col_pos, sums[1] - cnt * row_pos]
        totals = [t + jnp.sum(f, axis=1, keepdims=True) for t, f in zip(totals, feats)]
        n_loc = n_loc + jnp.sum(cnt, axis=1, keepdims=True)
        per_sweep.append(cents + [col_pos, row_pos])
        spot = ((row & 1) * 2 + (col & 1)) * plane
        spot = spot + lax.shift_right_logical(row, 1) * w2 + lax.shift_right_logical(col, 1)
        for k in range(4):
            ids = lax.broadcasted_iota(jnp.int32, (plane, pill), 0) + k * plane
            onehot[s, k * plane : (k + 1) * plane, :] = (ids == spot).astype(F32).astype(BF16)
    pw_cols = pw_t[...]
    m_loc = jnp.zeros((ch, 1), F32)
    for f in range(9):
        m_loc = m_loc + pw_cols[:, f : f + 1] * totals[f]
    m_loc = m_loc / n_loc
    for s in range(sweeps):
        base = -m_loc
        for f in range(5):
            base = base - pw_cols[:, f + 4 : f + 5] * per_sweep[s][f]
        bm[s] = base

    def one_channel(c, carry):
        wx = pw_s[0, c] + pw_s[4, c] + pw_s[7, c]
        wy = pw_s[1, c] + pw_s[5, c] + pw_s[8, c]
        wz = pw_s[2, c] + pw_s[6, c]
        wr = pw_s[3, c]
        total = jnp.zeros((8, pill), F32)
        for s in range(sweeps):
            most = jnp.full((8, pill), LOWEST, F32)
            shift = bm[s, pl.ds(c, 1), :]
            have = counts[s : s + 1, :]
            for k in range(maxp // 8):
                part = pl.ds(8 * k, 8)
                ids = lax.broadcasted_iota(jnp.int32, (8, pill), 0) + 8 * k
                ok = ids < have
                h = points[s, 0, part, :] * wx + points[s, 1, part, :] * wy
                h = h + points[s, 2, part, :] * wz + points[s, 3, part, :] * wr + shift
                most = jnp.maximum(most, jnp.where(ok, h, LOWEST))
                h = jnp.where(ok, h, 0.0)
                total = total + h * h
            mx[s, c] = most
        folded = total[:, 0:128]
        for t in range(1, pill // 128):
            folded = folded + total[:, t * 128 : (t + 1) * 128]
        sq[c] = folded
        return carry

    lax.fori_loop(0, ch, one_channel, 0)
    both = jnp.concatenate([jnp.broadcast_to(m_loc, (ch, 128)), jnp.sum(sq[...], axis=1)], axis=0)
    turned = both.T
    row = jnp.where(lane < ch, turned[0:1, :], jnp.sum(turned, axis=0, keepdims=True))
    row = jnp.concatenate([row, jnp.broadcast_to(n_loc, (1, 2 * ch))], axis=1)

    pl.semaphore_wait(barrier, n - 1)
    send_row(st0, 0, row)

    for layer in range(LAYERS):
        hi, lo = split(wf[layer])
        wfs[layer, 0:ch, :] = hi
        wfs[layer, ch : 2 * ch, :] = lo
    for layer in range(LAYERS - 1):
        hi, lo = split(wb[layer])
        wbs[layer, 0:ch, :] = hi
        wbs[layer, ch : 2 * ch, :] = lo
    hi, lo = split(wb0[...])
    wb0s[0 : 4 * ch, :] = hi
    wb0s[4 * ch : 8 * ch, :] = lo

    def columns(row):
        turned = jnp.broadcast_to(row, (8, 2 * ch)).T
        return turned[0:ch, 0:1], turned[ch : 2 * ch, 0:1]

    got = wait_row(st0, 0)
    n_all = jnp.sum(got[:, :, 2 * ch :], axis=0)
    rows = got[:, :, 0 : 2 * ch]
    weighted = got[:, :, 2 * ch :]
    means = jnp.sum(rows * weighted, axis=0) / n_all
    dev = rows - means[None]
    spread = jnp.sum(dev * dev * weighted, axis=0)
    second = (jnp.sum(rows, axis=0) + pltpu.roll(spread, ch, axis=1)) / n_all
    mean_c, inv_c = columns(jnp.where(lane < ch, means, lax.rsqrt(second + EPS)))
    scale_c = pfn_gb[:, 0:1] * inv_c
    shift_c = scale_c * (m_loc - mean_c) + pfn_gb[:, 1:2]

    ids = lax.broadcasted_iota(jnp.int32, (1, pix), 1)
    col_id = ids & (w2 - 1)
    row_id = lax.shift_right_logical(ids, w2.bit_length() - 1) & (h2 - 1)

    def moved(x, dr, dc):
        ok = None
        if dc == -1:
            ok = col_id >= 1
        elif dc == 1:
            ok = col_id < w2 - 1
        if dr == -1:
            rok = row_id >= 1
            ok = rok if ok is None else ok & rok
        elif dr == 1:
            rok = row_id < h2 - 1
            ok = rok if ok is None else ok & rok
        if ok is None:
            return x
        return jnp.where(ok, pltpu.roll(x, (-(dr * w2 + dc)) % pix, axis=1), 0.0)

    planes = [[], [], [], []]
    for s in range(sweeps):
        pillar = jnp.maximum(jnp.max(mx[s], axis=1) * scale_c + shift_c, 0.0)
        hi, lo = split(pillar)
        placed = dot(jnp.concatenate([hi, lo], axis=0), onehot[s], NT)
        for k in range(4):
            part = placed[:, k * plane : (k + 1) * plane]
            planes[k].append(part[0:ch] + part[ch : 2 * ch])
    planes = [jnp.concatenate(p, axis=1) for p in planes]
    for a in range(3):
        for b in range(3):
            which = (0 if a == 1 else 2) + (0 if b == 1 else 1)
            tap = moved(planes[which], -1 if a == 0 else 0, -1 if b == 0 else 0)
            hi, lo = split(tap)
            at = pl.ds((3 * a + b) * ch, ch)
            xs[0, 0, at, :] = hi
            xs[0, 1, at, :] = lo

    entries_loc = float(pix)
    entries = float(pix * n)

    def fold(x):
        out = x[:, 0:128]
        for t in range(1, pix // 128):
            out = out + x[:, t * 128 : (t + 1) * 128]
        return out

    for layer in range(LAYERS):
        big = dot(wfs[layer], xs[layer, 0])
        z = big[0:ch] + big[ch : 2 * ch] + dot(wfs[layer, 0:ch, :], xs[layer, 1])
        sums = fold(z)
        m_loc = jnp.sum(sums, axis=1, keepdims=True) / entries_loc
        d = z - m_loc
        turned = jnp.concatenate([sums, fold(d * d)], axis=0).T
        row = jnp.sum(turned, axis=0, keepdims=True)
        row = jnp.where(lane < ch, row / entries_loc, row)
        send_row(st, layer + 1, row)
        rows = wait_row(st, layer + 1)
        total = jnp.sum(rows, axis=0)
        means = total / float(n)
        dev = rows - means[None]
        spread = jnp.sum(dev * dev, axis=0) * entries_loc
        second = (total + pltpu.roll(spread, ch, axis=1)) / entries
        row = jnp.where(lane < ch, means, lax.rsqrt(second + EPS))
        mean_c, inv_c = columns(row)
        normed = (z - mean_c) * inv_c
        y = bn_cols[:, layer : layer + 1] * normed
        y = y + bn_cols[:, LAYERS + layer : LAYERS + layer + 1]
        xh[layer] = normed
        yy[layer] = y
        sq[layer, :, :] = jnp.broadcast_to(row, (8, 2 * ch))
        act = y * jax.nn.sigmoid(y)
        if layer + 1 < LAYERS:
            for a in range(3):
                for b in range(3):
                    hi, lo = split(moved(act, a - 1, b - 1))
                    at = pl.ds((3 * a + b) * ch, ch)
                    xs[layer + 1, 0, at, :] = hi
                    xs[layer + 1, 1, at, :] = lo
        else:
            for s in range(sweeps):
                for r in range(h2):
                    at = s * plane + r * w2
                    feat[s, :, r, :] = act[:, at : at + w2]

    def weight_grad(layer):
        both = gz_s[...]
        big = dot(both, xs[layer, 0], NT)
        dw = big[0:ch] + big[ch : 2 * ch] + dot(both[0:ch], xs[layer, 1], NT)
        for j in range(owners):
            rs[layer, j] = dw[j * rows_per : (j + 1) * rows_per, :]
        send_parts(layer)

    u = jnp.concatenate([cot[s, :, r, :] for s in range(sweeps) for r in range(h2)], axis=1)
    for layer in range(LAYERS - 1, -1, -1):
        y = yy[layer]
        normed = xh[layer]
        sig = jax.nn.sigmoid(y)
        gy = u * (sig * (1.0 + y * (1.0 - sig)))
        turned = jnp.concatenate([fold(gy), fold(gy * normed)], axis=0).T
        rnd = 2 * LAYERS - layer
        send_row(st, rnd, jnp.sum(turned, axis=0, keepdims=True))
        if layer < LAYERS - 1:
            weight_grad(layer + 1)
        if layer < LAYERS - 2:
            add_parts(layer + 2)
        row = jnp.sum(wait_row(st, rnd), axis=0)
        norms[0, layer : layer + 1, :] = row[:, ch : 2 * ch]
        norms[1, layer : layer + 1, :] = row[:, 0:ch]
        dy_c, dyx_c = columns(row / entries)
        inv_c = columns(sq[layer, 0:1, :])[1]
        gz = (bn_cols[:, layer : layer + 1] * inv_c) * (gy - dy_c - normed * dyx_c)
        hi, lo = split(gz)
        gz_s[0:ch, :] = hi
        gz_s[ch : 2 * ch, :] = lo
        if layer > 0:
            for a in range(3):
                for b in range(3):
                    hi, lo = split(moved(gz, 1 - a, 1 - b))
                    at = pl.ds((3 * a + b) * ch, ch)
                    gs[0, at, :] = hi
                    gs[1, at, :] = lo
            big = dot(wbs[layer - 1], gs[0])
            u = big[0:ch] + big[ch : 2 * ch] + dot(wbs[layer - 1, 0:ch, :], gs[1])
    weight_grad(0)
    add_parts(1)
    for dr in range(2):
        for dc in range(2):
            hi, lo = split(moved(gz, dr, dc))
            at = pl.ds((2 * dr + dc) * ch, ch)
            gs[0, at, :] = hi
            gs[1, at, :] = lo
    big = dot(wb0s[...], gs[0, 0 : 4 * ch, :])
    u0 = big[0 : 4 * ch] + big[4 * ch :] + dot(wb0s[0 : 4 * ch, :], gs[1, 0 : 4 * ch, :])
    for s in range(sweeps):
        total = None
        for k in range(4):
            hi, lo = split(u0[k * ch : (k + 1) * ch, s * plane : (s + 1) * plane])
            part = dot(
                jnp.concatenate([hi, lo], axis=0), onehot[s, k * plane : (k + 1) * plane, :]
            )
            total = part if total is None else total + part
        pgrad[s] = total[0:ch] + total[ch : 2 * ch]
    add_parts(0)

    for layer in range(LAYERS):
        others = grads.at[layer, pl.ds(0, owners - 1)]
        if owners == n:
            pltpu.make_async_copy(others, others, ag_recv.at[layer]).wait()
        else:
            all_of = grads.at[layer]

            @pl.when(me < owners)
            def _():
                pltpu.make_async_copy(others, others, ag_recv.at[layer]).wait()

            @pl.when(me >= owners)
            def _():
                pltpu.make_async_copy(all_of, all_of, ag_recv.at[layer]).wait()

    for rnd in range(2 * LAYERS + 1):
        most = (st0.at[0] if rnd == 0 else st.at[rnd]).at[pl.ds(0, n - 1)]
        pltpu.make_async_copy(most, most, st_send.at[rnd]).wait()
    for layer in range(LAYERS):
        others = rs.at[layer, pl.ds(0, owners - 1)]
        sent = rbuf.at[layer, pl.ds(0, n - 1)]
        if owners == n:
            pltpu.make_async_copy(others, others, rs_send.at[layer]).wait()
            pltpu.make_async_copy(sent, sent, ag_send.at[layer]).wait()
        else:
            all_of = rs.at[layer]

            @pl.when(me < owners)
            def _():
                pltpu.make_async_copy(others, others, rs_send.at[layer]).wait()
                pltpu.make_async_copy(sent, sent, ag_send.at[layer]).wait()

            @pl.when(me >= owners)
            def _():
                pltpu.make_async_copy(all_of, all_of, rs_send.at[layer]).wait()


def per_device(
    n_rack,
    n_chip,
    points,
    counts,
    cells,
    pfn_weight,
    pfn_gain,
    pfn_bias,
    conv_weight,
    bn_gain,
    bn_bias,
    cotangent,
):
    sweeps, _, maxp, pill = points.shape
    ch = pfn_weight.shape[1]
    h2, w2 = cotangent.shape[2:]
    gh, gw = 2 * h2, 2 * w2
    n = n_rack * n_chip
    owners = min(n, ch)
    rows_per = ch // owners
    pix = sweeps * h2 * w2
    kdim = 9 * ch
    taps = conv_weight.reshape(LAYERS, 9, ch, ch)
    wf = taps.transpose(0, 2, 1, 3).reshape(LAYERS, ch, kdim)
    wb = taps[1:].transpose(0, 3, 1, 2).reshape(LAYERS - 1, ch, kdim)
    first = taps[0].transpose(0, 2, 1)
    zero = jnp.zeros((ch, ch), F32)
    tap_of = {(0, 0): 1, (1, 0): 2, (1, 1): 0}
    blocks = []
    for row_par in range(2):
        for col_par in range(2):
            line = []
            for dr in range(2):
                for dc in range(2):
                    a, b = tap_of.get((row_par, dr)), tap_of.get((col_par, dc))
                    line.append(zero if a is None or b is None else first[3 * a + b])
            blocks.append(line)
    wb0 = jnp.block(blocks)
    dims = (n_rack, n_chip, sweeps, maxp, gh, gw, pill, ch, owners)
    vmem = pl.BlockSpec(memory_space=pltpu.VMEM)
    smem = pl.BlockSpec(memory_space=pltpu.SMEM)
    feat, grads, norms, pgrad = pl.pallas_call(
        functools.partial(kernel, dims),
        out_shape=(
            jax.ShapeDtypeStruct((sweeps, ch, h2, w2), F32),
            jax.ShapeDtypeStruct((LAYERS, owners, rows_per, kdim), F32),
            jax.ShapeDtypeStruct((2, LAYERS, ch), F32),
            jax.ShapeDtypeStruct((sweeps, ch, pill), F32),
        ),
        in_specs=[vmem, vmem, vmem, smem] + [vmem] * 7,
        out_specs=(vmem, vmem, vmem, vmem),
        scratch_shapes=[
            pltpu.VMEM((LAYERS, 2, kdim, pix), BF16),
            pltpu.VMEM((2, kdim, pix), BF16),
            pltpu.VMEM((LAYERS, 2 * ch, kdim), BF16),
            pltpu.VMEM((LAYERS - 1, 2 * ch, kdim), BF16),
            pltpu.VMEM((8 * ch, 4 * ch), BF16),
            pltpu.VMEM((sweeps, gh * gw, pill), BF16),
            pltpu.VMEM((sweeps, ch, pill), F32),
            pltpu.VMEM((sweeps, ch, 8, pill), F32),
            pltpu.VMEM((ch, 8, 128), F32),
            pltpu.VMEM((LAYERS, ch, pix), F32),
            pltpu.VMEM((LAYERS, ch, pix), F32),
            pltpu.VMEM((2 * ch, pix), BF16),
            pltpu.VMEM((1, n, 1, 4 * ch), F32),
            pltpu.VMEM((2 * LAYERS + 1, n, 1, 2 * ch), F32),
            pltpu.VMEM((LAYERS, owners, rows_per, kdim), F32),
            pltpu.VMEM((LAYERS, n, rows_per, kdim), F32),
            pltpu.SemaphoreType.DMA((2 * LAYERS + 1,)),
            pltpu.SemaphoreType.DMA((2 * LAYERS + 1,)),
            pltpu.SemaphoreType.DMA((LAYERS,)),
            pltpu.SemaphoreType.DMA((LAYERS,)),
            pltpu.SemaphoreType.DMA((LAYERS,)),
            pltpu.SemaphoreType.DMA((LAYERS,)),
        ],
        compiler_params=pltpu.CompilerParams(
            collective_id=0, has_side_effects=True, vmem_limit_bytes=60 * 1024 * 1024
        ),
    )(
        points,
        counts,
        cells,
        pfn_weight,
        pfn_weight.T,
        jnp.stack([pfn_gain, pfn_bias], axis=1),
        wf,
        wb,
        wb0,
        jnp.concatenate([bn_gain, bn_bias], axis=0).T,
        cotangent,
    )
    grads = grads.reshape(LAYERS, ch, 9, ch).transpose(0, 2, 1, 3)
    return (feat, grads.reshape(LAYERS, 9, ch * ch), norms, pgrad)


def solution(mesh):
    both = ("rack", "chip")
    return jax.shard_map(
        functools.partial(per_device, mesh.shape["rack"], mesh.shape["chip"]),
        mesh=mesh,
        in_specs=(
            P(both, None, None, None),
            P(both, None),
            P(both, None),
            P(),
            P(),
            P(),
            P(),
            P(),
            P(),
            P(both, None, None, None),
        ),
        out_specs=(
            P(both, None, None, None),
            P(),
            P(),
            P(both, None, None),
        ),
        check_vma=False,
    )
```

```python
import functools

import jax
import jax.numpy as jnp
from jax import lax
from jax.experimental import pallas as pl
from jax.experimental.pallas import tpu as pltpu
from jax.sharding import PartitionSpec as P

LAYERS = 4
EPS = 1e-05
F32 = jnp.float32
BF16 = jnp.bfloat16
NN = (((1,), (0,)), ((), ()))
NT = (((1,), (1,)), ((), ()))
LOWEST = -3e38


class Peer:
    def __init__(self, rack, chip, index):
        self.rack, self.chip, self.index = rack, chip, index


def dot(a, b, dims=NN):
    return lax.dot_general(a, b, dims, preferred_element_type=F32)


def split(x):
    hi = x.astype(BF16)
    lo = (x - hi.astype(F32)).astype(BF16)
    return hi, lo


def kernel(
    dims,
    points,
    counts,
    cells,
    pw_s,
    pw,
    pfn_gain,
    pfn_bias,
    w4,
    bn_gain,
    bn_bias,
    cot,
    feat,
    out_g,
    norms,
    pgrad,
    xs,
    gs,
    wfs,
    wbs,
    wb0s,
    onehot,
    par,
    cot_s,
    grads,
    bm,
    mx,
    sq,
    xh,
    yy,
    gz_s,
    st0,
    st,
    rs,
    rbuf,
    st_send,
    st_recv,
    rs_send,
    rs_recv,
    ag_send,
    ag_recv,
):
    n_rack, n_chip, sweeps, maxp, gh, gw, pill, ch, owners = dims
    n = n_rack * n_chip
    h2, w2 = gh // 2, gw // 2
    plane = h2 * w2
    pix = sweeps * plane
    rows_per = ch // owners
    kdim = 9 * ch
    my_rack, my_chip = lax.axis_index("rack"), lax.axis_index("chip")
    me = my_rack * n_chip + my_chip

    def device(t):
        if isinstance(t, Peer):
            return {"rack": t.rack, "chip": t.chip}
        return {"rack": lax.div(t, n_chip), "chip": lax.rem(t, n_chip)}

    def far(k):
        dr, dc = divmod(k, n_chip)
        return -min(dc, n_chip - dc) - min(dr, n_rack - dr)

    def peers(body):
        if n <= 32:
            for k in sorted(range(1, n), key=far):
                dr, dc = divmod(k, n_chip)
                rack = lax.rem(my_rack + dr, n_rack) if dr else my_rack
                chip = lax.rem(my_chip + dc, n_chip) if dc else my_chip
                body(Peer(rack, chip, rack * n_chip + chip))
            return

        def step(k, carry):
            body(lax.rem(me + k, n))
            return carry

        lax.fori_loop(1, n, step, 0)

    barrier = pltpu.get_barrier_semaphore()
    peers(
        lambda t: pl.semaphore_signal(
            barrier, inc=1, device_id=device(t), device_id_type=pl.DeviceIdType.MESH
        )
    )

    def send_row(buf, rnd, row):
        buf[rnd, me] = row

        def go(t):
            pltpu.make_async_remote_copy(
                src_ref=buf.at[rnd, me],
                dst_ref=buf.at[rnd, me],
                send_sem=st_send.at[rnd],
                recv_sem=st_recv.at[rnd],
                device_id=device(t),
                device_id_type=pl.DeviceIdType.MESH,
            ).start()

        peers(go)

    def wait_row(buf, rnd):
        most = buf.at[rnd, pl.ds(0, n - 1)]
        pltpu.make_async_copy(most, most, st_recv.at[rnd]).wait()
        return buf[rnd]

    def send_parts(layer):
        def go(t):
            def copy():
                pltpu.make_async_remote_copy(
                    src_ref=rs.at[layer, t.index if isinstance(t, Peer) else t],
                    dst_ref=rbuf.at[layer, me],
                    send_sem=rs_send.at[layer],
                    recv_sem=rs_recv.at[layer],
                    device_id=device(t),
                    device_id_type=pl.DeviceIdType.MESH,
                ).start()

            if owners == n:
                copy()
            else:
                pl.when(t < owners)(copy)

        peers(go)

    def when_owner(body):
        if owners == n:
            body()
        else:
            pl.when(me < owners)(body)

    def add_parts(layer):
        def body():
            most = rbuf.at[layer, pl.ds(0, n - 1)]
            pltpu.make_async_copy(most, most, rs_recv.at[layer]).wait()
            rbuf[layer, me] = rs[layer, me]
            grads[layer, me] = jnp.sum(rbuf[layer], axis=0)

            def go(t):
                pltpu.make_async_remote_copy(
                    src_ref=grads.at[layer, me],
                    dst_ref=grads.at[layer, me],
                    send_sem=ag_send.at[layer],
                    recv_sem=ag_recv.at[layer],
                    device_id=device(t),
                    device_id_type=pl.DeviceIdType.MESH,
                ).start()

            peers(go)

        when_owner(body)

    slot = lax.broadcasted_iota(jnp.int32, (maxp, pill), 0)
    lane = lax.broadcasted_iota(jnp.int32, (1, 2 * ch), 1)
    per_sweep = []
    spots = []
    totals = [jnp.zeros((1, 1), F32)] * 9
    n_loc = jnp.zeros((1, 1), F32)
    for s in range(sweeps):
        valid = slot < counts[s : s + 1, :]
        mask = valid.astype(F32)
        cnt = counts[s : s + 1, :].astype(F32)
        sums = [jnp.sum(points[s, f] * mask, axis=0, keepdims=True) for f in range(4)]
        cents = [sums[f] / cnt for f in range(3)]
        cell = cells[s : s + 1, :]
        row = lax.shift_right_logical(cell, gw.bit_length() - 1)
        col = cell & (gw - 1)
        col_pos = col.astype(F32) * (2.0 / gw) - 1.0
        row_pos = row.astype(F32) * (2.0 / gh) - 1.0
        feats = sums + [sums[f] - cnt * cents[f] for f in range(3)]
        feats += [sums[0] - cnt * col_pos, sums[1] - cnt * row_pos]
        totals = [t + jnp.sum(f, axis=1, keepdims=True) for t, f in zip(totals, feats)]
        n_loc = n_loc + jnp.sum(cnt, axis=1, keepdims=True)
        per_sweep.append(cents + [col_pos, row_pos])
        spot = ((row & 1) * 2 + (col & 1)) * plane
        spot = spot + lax.shift_right_logical(row, 1) * w2 + lax.shift_right_logical(col, 1)
        spots.append(spot)
    par[...] = jnp.zeros(par.shape, F32)
    par[0:9, 0:ch] = pw[...]
    par[9:10, 0:ch] = pfn_gain[...]
    par[10:11, 0:ch] = pfn_bias[...]
    par[11 : 11 + LAYERS, 0:ch] = bn_gain[...]
    par[11 + LAYERS : 11 + 2 * LAYERS, 0:ch] = bn_bias[...]
    par_cols = par[...].T
    pw_cols = par_cols[0:ch, 0:9]
    gain_c, bias_c = par_cols[0:ch, 9:10], par_cols[0:ch, 10:11]
    bn_cols = par_cols[0:ch, 11 : 11 + 2 * LAYERS]
    m_loc = jnp.zeros((ch, 1), F32)
    for f in range(9):
        m_loc = m_loc + pw_cols[:, f : f + 1] * totals[f]
    m_loc = m_loc / n_loc
    for s in range(sweeps):
        base = -m_loc
        for f in range(5):
            base = base - pw_cols[:, f + 4 : f + 5] * per_sweep[s][f]
        bm[s] = base

    def one_channel(c, carry):
        wx = pw_s[0, c] + pw_s[4, c] + pw_s[7, c]
        wy = pw_s[1, c] + pw_s[5, c] + pw_s[8, c]
        wz = pw_s[2, c] + pw_s[6, c]
        wr = pw_s[3, c]
        total = jnp.zeros((8, pill), F32)
        for s in range(sweeps):
            most = jnp.full((8, pill), LOWEST, F32)
            shift = bm[s, pl.ds(c, 1), :]
            have = counts[s : s + 1, :]
            for k in range(maxp // 8):
                part = pl.ds(8 * k, 8)
                ids = lax.broadcasted_iota(jnp.int32, (8, pill), 0) + 8 * k
                ok = ids < have
                h = points[s, 0, part, :] * wx + points[s, 1, part, :] * wy
                h = h + points[s, 2, part, :] * wz + points[s, 3, part, :] * wr + shift
                most = jnp.maximum(most, jnp.where(ok, h, LOWEST))
                h = jnp.where(ok, h, 0.0)
                total = total + h * h
            mx[s, c] = most
        folded = total[:, 0:128]
        for t in range(1, pill // 128):
            folded = folded + total[:, t * 128 : (t + 1) * 128]
        sq[c] = folded
        return carry

    lax.fori_loop(0, ch, one_channel, 0)
    both = jnp.concatenate([jnp.broadcast_to(m_loc, (ch, 128)), jnp.sum(sq[...], axis=1)], axis=0)
    turned = both.T
    row = jnp.where(lane < ch, turned[0:1, :], jnp.sum(turned, axis=0, keepdims=True))
    row = jnp.concatenate([row, jnp.broadcast_to(n_loc, (1, 2 * ch))], axis=1)

    pl.semaphore_wait(barrier, n - 1)
    send_row(st0, 0, row)

    def forward_weights(layer):
        w = [w4[layer, t * ch : (t + 1) * ch, :] for t in range(9)]
        hi, lo = split(jnp.concatenate(w, axis=1))
        wfs[layer, 0:ch, :] = hi
        wfs[layer, ch : 2 * ch, :] = lo

    def backward_weights(layer):
        hi, lo = split(w4[layer].T)
        wbs[layer - 1, 0:ch, :] = hi
        wbs[layer - 1, ch : 2 * ch, :] = lo

    def first_backward_weights():
        w = w4[0].T
        zero = jnp.zeros((ch, ch), F32)
        tap_of = {(0, 0): 1, (1, 0): 2, (1, 1): 0}
        for k in range(4):
            line = []
            for j in range(4):
                a, b = tap_of.get((k // 2, j // 2)), tap_of.get((k % 2, j % 2))
                t = None if a is None or b is None else 3 * a + b
                line.append(zero if t is None else w[:, t * ch : (t + 1) * ch])
            hi, lo = split(jnp.concatenate(line, axis=1))
            wb0s[k * ch : (k + 1) * ch, :] = hi
            wb0s[(4 + k) * ch : (5 + k) * ch, :] = lo

    for s in range(sweeps):
        for k in range(4):
            ids = lax.broadcasted_iota(jnp.int32, (plane, pill), 0) + k * plane
            onehot[s, k * plane : (k + 1) * plane, :] = (ids == spots[s]).astype(F32).astype(BF16)
    for s in range(sweeps):
        bm[s] = jnp.max(mx[s], axis=1)
    forward_weights(0)

    def columns(row):
        turned = jnp.broadcast_to(row, (8, 2 * ch)).T
        return turned[0:ch, 0:1], turned[ch : 2 * ch, 0:1]

    got = wait_row(st0, 0)
    n_all = jnp.sum(got[:, :, 2 * ch :], axis=0)
    rows = got[:, :, 0 : 2 * ch]
    weighted = got[:, :, 2 * ch :]
    means = jnp.sum(rows * weighted, axis=0) / n_all
    dev = rows - means[None]
    spread = jnp.sum(dev * dev * weighted, axis=0)
    second = (jnp.sum(rows, axis=0) + pltpu.roll(spread, ch, axis=1)) / n_all
    mean_c, inv_c = columns(jnp.where(lane < ch, means, lax.rsqrt(second + EPS)))
    scale_c = gain_c * inv_c
    shift_c = scale_c * (m_loc - mean_c) + bias_c

    ids = lax.broadcasted_iota(jnp.int32, (1, pix), 1)
    col_id = ids & (w2 - 1)
    row_id = lax.shift_right_logical(ids, w2.bit_length() - 1) & (h2 - 1)

    def moved(x, dr, dc):
        ok = None
        if dc == -1:
            ok = col_id >= 1
        elif dc == 1:
            ok = col_id < w2 - 1
        if dr == -1:
            rok = row_id >= 1
            ok = rok if ok is None else ok & rok
        elif dr == 1:
            rok = row_id < h2 - 1
            ok = rok if ok is None else ok & rok
        if ok is None:
            return x
        return jnp.where(ok, pltpu.roll(x, (-(dr * w2 + dc)) % pix, axis=1), 0.0)

    planes = [[], [], [], []]
    for s in range(sweeps):
        pillar = jnp.maximum(bm[s] * scale_c + shift_c, 0.0)
        hi, lo = split(pillar)
        placed = dot(jnp.concatenate([hi, lo], axis=0), onehot[s], NT)
        for k in range(4):
            part = placed[:, k * plane : (k + 1) * plane]
            planes[k].append(part[0:ch] + part[ch : 2 * ch])
    planes = [jnp.concatenate(p, axis=1) for p in planes]
    for a in range(3):
        for b in range(3):
            which = (0 if a == 1 else 2) + (0 if b == 1 else 1)
            tap = moved(planes[which], -1 if a == 0 else 0, -1 if b == 0 else 0)
            hi, lo = split(tap)
            at = pl.ds((3 * a + b) * ch, ch)
            xs[0, 0, at, :] = hi
            xs[0, 1, at, :] = lo

    entries_loc = float(pix)
    entries = float(pix * n)

    def fold(x):
        out = x[:, 0:128]
        for t in range(1, pix // 128):
            out = out + x[:, t * 128 : (t + 1) * 128]
        return out

    def slope(y):
        sig = jax.nn.sigmoid(y)
        return sig * (1.0 + y * (1.0 - sig))

    for layer in range(LAYERS):
        big = dot(wfs[layer], xs[layer, 0])
        z = big[0:ch] + big[ch : 2 * ch] + dot(wfs[layer, 0:ch, :], xs[layer, 1])
        sums = fold(z)
        m_loc = jnp.sum(sums, axis=1, keepdims=True) / entries_loc
        d = z - m_loc
        turned = jnp.concatenate([sums, fold(d * d)], axis=0).T
        row = jnp.sum(turned, axis=0, keepdims=True)
        row = jnp.where(lane < ch, row / entries_loc, row)
        send_row(st, layer + 1, row)
        if layer == 0:
            first_backward_weights()
        else:
            backward_weights(layer)
            yy[layer - 1] = slope(yy[layer - 1])
        if layer + 1 < LAYERS:
            forward_weights(layer + 1)
        else:
            for s in range(sweeps):
                for r in range(h2):
                    at = s * plane + r * w2
                    cot_s[:, at : at + w2] = cot[s, :, r, :]
        rows = wait_row(st, layer + 1)
        total = jnp.sum(rows, axis=0)
        means = total / float(n)
        dev = rows - means[None]
        spread = jnp.sum(dev * dev, axis=0) * entries_loc
        second = (total + pltpu.roll(spread, ch, axis=1)) / entries
        row = jnp.where(lane < ch, means, lax.rsqrt(second + EPS))
        mean_c, inv_c = columns(row)
        normed = (z - mean_c) * inv_c
        y = bn_cols[:, layer : layer + 1] * normed
        y = y + bn_cols[:, LAYERS + layer : LAYERS + layer + 1]
        xh[layer] = normed
        sq[layer, :, :] = jnp.broadcast_to(row, (8, 2 * ch))
        sig = jax.nn.sigmoid(y)
        act = y * sig
        yy[layer] = y if layer + 1 < LAYERS else sig * (1.0 + y * (1.0 - sig))
        if layer + 1 < LAYERS:
            for a in range(3):
                for b in range(3):
                    hi, lo = split(moved(act, a - 1, b - 1))
                    at = pl.ds((3 * a + b) * ch, ch)
                    xs[layer + 1, 0, at, :] = hi
                    xs[layer + 1, 1, at, :] = lo

    def weight_grad(layer):
        both = gz_s[...]
        big = dot(both, xs[layer, 0], NT)
        dw = big[0:ch] + big[ch : 2 * ch] + dot(both[0:ch], xs[layer, 1], NT)
        for j in range(owners):
            rs[layer, j] = dw[j * rows_per : (j + 1) * rows_per, :]
        send_parts(layer)

    u = cot_s[...]
    for layer in range(LAYERS - 1, -1, -1):
        normed = xh[layer]
        gy = u * yy[layer]
        turned = jnp.concatenate([fold(gy), fold(gy * normed)], axis=0).T
        rnd = 2 * LAYERS - layer
        send_row(st, rnd, jnp.sum(turned, axis=0, keepdims=True))
        if layer == LAYERS - 1:
            for s in range(sweeps):
                for r in range(h2):
                    at = s * plane + r * w2
                    feat[s, :, r, :] = act[:, at : at + w2]
        if layer < LAYERS - 1:
            weight_grad(layer + 1)
        if layer < LAYERS - 2:
            add_parts(layer + 2)
        row = jnp.sum(wait_row(st, rnd), axis=0)
        norms[0, layer : layer + 1, :] = row[:, ch : 2 * ch]
        norms[1, layer : layer + 1, :] = row[:, 0:ch]
        dy_c, dyx_c = columns(row / entries)
        inv_c = columns(sq[layer, 0:1, :])[1]
        gz = (bn_cols[:, layer : layer + 1] * inv_c) * (gy - dy_c - normed * dyx_c)
        hi, lo = split(gz)
        gz_s[0:ch, :] = hi
        gz_s[ch : 2 * ch, :] = lo
        if layer > 0:
            for a in range(3):
                for b in range(3):
                    hi, lo = split(moved(gz, 1 - a, 1 - b))
                    at = pl.ds((3 * a + b) * ch, ch)
                    gs[0, at, :] = hi
                    gs[1, at, :] = lo
            big = dot(wbs[layer - 1], gs[0])
            u = big[0:ch] + big[ch : 2 * ch] + dot(wbs[layer - 1, 0:ch, :], gs[1])
    weight_grad(0)
    add_parts(1)
    for dr in range(2):
        for dc in range(2):
            hi, lo = split(moved(gz, dr, dc))
            at = pl.ds((2 * dr + dc) * ch, ch)
            gs[0, at, :] = hi
            gs[1, at, :] = lo
    big = dot(wb0s[...], gs[0, 0 : 4 * ch, :])
    u0 = big[0 : 4 * ch] + big[4 * ch :] + dot(wb0s[0 : 4 * ch, :], gs[1, 0 : 4 * ch, :])
    for s in range(sweeps):
        total = None
        for k in range(4):
            hi, lo = split(u0[k * ch : (k + 1) * ch, s * plane : (s + 1) * plane])
            part = dot(
                jnp.concatenate([hi, lo], axis=0), onehot[s, k * plane : (k + 1) * plane, :]
            )
            total = part if total is None else total + part
        pgrad[s] = total[0:ch] + total[ch : 2 * ch]
    add_parts(0)

    for layer in range(LAYERS - 1, -1, -1):
        others = grads.at[layer, pl.ds(0, owners - 1)]
        if owners == n:
            pltpu.make_async_copy(others, others, ag_recv.at[layer]).wait()
        else:
            all_of = grads.at[layer]

            @pl.when(me < owners)
            def _():
                pltpu.make_async_copy(others, others, ag_recv.at[layer]).wait()

            @pl.when(me >= owners)
            def _():
                pltpu.make_async_copy(all_of, all_of, ag_recv.at[layer]).wait()

        whole = grads[layer].reshape(ch, kdim)
        for t in range(9):
            out_g[layer, t] = whole[:, t * ch : (t + 1) * ch]

    for rnd in range(2 * LAYERS + 1):
        most = (st0.at[0] if rnd == 0 else st.at[rnd]).at[pl.ds(0, n - 1)]
        pltpu.make_async_copy(most, most, st_send.at[rnd]).wait()
    for layer in range(LAYERS):
        others = rs.at[layer, pl.ds(0, owners - 1)]
        sent = rbuf.at[layer, pl.ds(0, n - 1)]
        if owners == n:
            pltpu.make_async_copy(others, others, rs_send.at[layer]).wait()
            pltpu.make_async_copy(sent, sent, ag_send.at[layer]).wait()
        else:
            all_of = rs.at[layer]

            @pl.when(me < owners)
            def _():
                pltpu.make_async_copy(others, others, rs_send.at[layer]).wait()
                pltpu.make_async_copy(sent, sent, ag_send.at[layer]).wait()

            @pl.when(me >= owners)
            def _():
                pltpu.make_async_copy(all_of, all_of, rs_send.at[layer]).wait()


def per_device(
    n_rack,
    n_chip,
    points,
    counts,
    cells,
    pfn_weight,
    pfn_gain,
    pfn_bias,
    conv_weight,
    bn_gain,
    bn_bias,
    cotangent,
):
    sweeps, _, maxp, pill = points.shape
    ch = pfn_weight.shape[1]
    h2, w2 = cotangent.shape[2:]
    gh, gw = 2 * h2, 2 * w2
    n = n_rack * n_chip
    owners = min(n, ch)
    rows_per = ch // owners
    pix = sweeps * h2 * w2
    kdim = 9 * ch
    dims = (n_rack, n_chip, sweeps, maxp, gh, gw, pill, ch, owners)
    vmem = pl.BlockSpec(memory_space=pltpu.VMEM)
    smem = pl.BlockSpec(memory_space=pltpu.SMEM)
    feat, out_g, norms, pgrad = pl.pallas_call(
        functools.partial(kernel, dims),
        out_shape=(
            jax.ShapeDtypeStruct((sweeps, ch, h2, w2), F32),
            jax.ShapeDtypeStruct((LAYERS, 9, ch, ch), F32),
            jax.ShapeDtypeStruct((2, LAYERS, ch), F32),
            jax.ShapeDtypeStruct((sweeps, ch, pill), F32),
        ),
        in_specs=[vmem, vmem, vmem, smem] + [vmem] * 7,
        out_specs=(vmem, vmem, vmem, vmem),
        scratch_shapes=[
            pltpu.VMEM((LAYERS, 2, kdim, pix), BF16),
            pltpu.VMEM((2, kdim, pix), BF16),
            pltpu.VMEM((LAYERS, 2 * ch, kdim), BF16),
            pltpu.VMEM((LAYERS - 1, 2 * ch, kdim), BF16),
            pltpu.VMEM((8 * ch, 4 * ch), BF16),
            pltpu.VMEM((sweeps, gh * gw, pill), BF16),
            pltpu.VMEM((32, 128), F32),
            pltpu.VMEM((ch, pix), F32),
            pltpu.VMEM((LAYERS, owners, rows_per, kdim), F32),
            pltpu.VMEM((sweeps, ch, pill), F32),
            pltpu.VMEM((sweeps, ch, 8, pill), F32),
            pltpu.VMEM((ch, 8, 128), F32),
            pltpu.VMEM((LAYERS, ch, pix), F32),
            pltpu.VMEM((LAYERS, ch, pix), F32),
            pltpu.VMEM((2 * ch, pix), BF16),
            pltpu.VMEM((1, n, 1, 4 * ch), F32),
            pltpu.VMEM((2 * LAYERS + 1, n, 1, 2 * ch), F32),
            pltpu.VMEM((LAYERS, owners, rows_per, kdim), F32),
            pltpu.VMEM((LAYERS, n, rows_per, kdim), F32),
            pltpu.SemaphoreType.DMA((2 * LAYERS + 1,)),
            pltpu.SemaphoreType.DMA((2 * LAYERS + 1,)),
            pltpu.SemaphoreType.DMA((LAYERS,)),
            pltpu.SemaphoreType.DMA((LAYERS,)),
            pltpu.SemaphoreType.DMA((LAYERS,)),
            pltpu.SemaphoreType.DMA((LAYERS,)),
        ],
        compiler_params=pltpu.CompilerParams(
            collective_id=0, has_side_effects=True, vmem_limit_bytes=60 * 1024 * 1024
        ),
    )(
        points,
        counts,
        cells,
        pfn_weight,
        pfn_weight,
        pfn_gain.reshape(1, ch),
        pfn_bias.reshape(1, ch),
        conv_weight.reshape(LAYERS, kdim, ch),
        bn_gain,
        bn_bias,
        cotangent,
    )
    return (feat, out_g.reshape(LAYERS, 9, ch * ch), norms, pgrad)


def solution(mesh):
    both = ("rack", "chip")
    return jax.shard_map(
        functools.partial(per_device, mesh.shape["rack"], mesh.shape["chip"]),
        mesh=mesh,
        in_specs=(
            P(both, None, None, None),
            P(both, None),
            P(both, None),
            P(),
            P(),
            P(),
            P(),
            P(),
            P(),
            P(both, None, None, None),
        ),
        out_specs=(
            P(both, None, None, None),
            P(),
            P(),
            P(both, None, None),
        ),
        check_vma=False,
    )
```
